32 devices in a mesh: row: 8 (over y, x, core), col: 4 (over z).
Axes of the slice: x: 2, y: 2, z: 4, core: 2. Of those that a mesh axis runs over, the one named last changes fastest.
Arguments:
- positions: float32 [3, 16384], P(None, ('row', 'col')), may hold values from -6 to 6
- velocities: float32 [3, 16384], P(None, ('row', 'col')), may hold values from -6 to 6
- accels: float32 [3, 16384], P(None, ('row', 'col')), may hold values from -0.75 to 0.75
- jerks: float32 [3, 16384], P(None, ('row', 'col')), may hold values from -1.5 to 1.5
- masses: float32 [16384], P(('row', 'col')), may hold values from 0.3 to 3
- elapsed: float32 [16384], P(('row', 'col')), may hold values from 0.05 to 0.5
- active_star: int32 [1024], replicated, may hold values from 0 to 16383, as said below
Outputs:
- new_positions: float32 [3, 16384], P(None, ('row', 'col'))
- new_velocities: float32 [3, 16384], P(None, ('row', 'col'))
- new_accels: float32 [3, 16384], P(None, ('row', 'col'))
- new_jerks: float32 [3, 16384], P(None, ('row', 'col'))
The draws below stay inside these ranges and needn't reach their ends.
Inputs may be any that keep to these rules, and one draw needn't show every extreme that they name: `active_star`: the 1024 ids are distinct. Star g is owned by device g // 512, devices counted with row slowest and col fastest. In each aligned block of 128 entries (one group of targets), at most 48 entries name stars whose owning device has the same col index, and in every block some col index has exactly 48.
All inputs are finite; a program needn't handle non-finite values.
Results may differ from the reference program's by a relative error of at most 0.0003.
Values sent between devices are 32-bit elements; how exact they have to be, the bound alone decides.
No kernel may reach another device: no remote copies, remote signals or barrier semaphores. Data moves between devices by JAX's collectives and lax.ppermute only.
A program may use at most 64 MiB of HBM per device.

```python
import math
import jax
import jax.numpy as jnp
from jax import lax

STAR_DEV = 512
I_DEV = 128
CAP = 48
NSTARS = 16384
ACTIVE = 1024


def clump_layout(key):
    clump_count = max(NSTARS // 512, 4)
    layout_key = jax.random.fold_in(key, 7001)
    key_member, key_centre, key_width, key_drift = jax.random.split(layout_key, 4)
    member = jax.random.randint(key_member, (NSTARS,), 0, clump_count)
    centres = jax.random.normal(key_centre, (3, clump_count), jnp.float32)
    log_width = jax.random.uniform(key_width, (clump_count,), jnp.float32, jnp.log(0.04), jnp.log(0.12))
    drift_speed = 0.4 * jax.random.normal(key_drift, (3, clump_count), jnp.float32)
    return (member, centres, jnp.exp(log_width), drift_speed)


def draw_positions(key, part):
    member, centres, widths, drift_speed = clump_layout(key)
    offsets = jax.random.normal(jax.random.fold_in(key, 7002), (3, NSTARS), jnp.float32)
    placed = jnp.take(centres, member, axis=1) + jnp.take(widths, member)[None, :] * offsets
    return jnp.clip(placed, -6.0, 6.0).astype(jnp.float32)


def draw_velocities(key, part):
    member, centres, widths, drift_speed = clump_layout(key)
    inner_key = jax.random.fold_in(key, 7003)
    scatter = 0.3 * jax.random.normal(inner_key, (3, NSTARS), jnp.float32)
    moving = jnp.take(drift_speed, member, axis=1) + scatter
    return jnp.clip(moving, -6.0, 6.0).astype(jnp.float32)


def draw_active_star(key, part):
    rows_axis = ACTIVE // I_DEV
    cols_axis = NSTARS // (STAR_DEV * rows_axis)
    slots_all = cols_axis * CAP
    first_key, second_key = jax.random.split(key)

    def choose(subkey):
        key_full, key_score, key_order = jax.random.split(subkey, 3)
        forced = jax.random.randint(key_full, (), 0, cols_axis)
        serial = jnp.arange(slots_all, dtype=jnp.int32)
        scores = jax.random.randint(key_score, (slots_all,), 0, 1 << 20) * slots_all + serial
        scores = jnp.where(serial // CAP == forced, serial - slots_all, scores)
        chosen = jnp.argsort(scores, stable=True)[:I_DEV]
        return chosen[jax.random.permutation(key_order, I_DEV)]
    picked = jax.vmap(choose)(jax.random.split(first_key, rows_axis))
    column = picked // CAP
    within = picked % CAP
    blockno = jnp.arange(rows_axis, dtype=jnp.int32)[:, None]
    orders = jax.vmap(lambda subkey: jax.random.permutation(subkey, rows_axis * STAR_DEV))(jax.random.split(second_key, cols_axis))
    position = orders[column, blockno * CAP + within]
    owner_row = position // STAR_DEV
    return ((owner_row * cols_axis + column) * STAR_DEV + position % STAR_DEV).reshape(-1).astype(jnp.int32)


def level_of(rng, shape, cuts, low, top_value):
    def one(dim, shards_of):
        draws = jax.random.uniform(jax.random.fold_in(jax.random.fold_in(rng, 6), dim), (shards_of,), jnp.float32, low / len(cuts), top_value / len(cuts))
        return jnp.repeat(jnp.exp(draws), shape[dim] // shards_of).reshape((-1,) + (1,) * (len(shape) - dim - 1))

    factor_of = one(*cuts[0])
    for cut in cuts[1:]:
        factor_of = factor_of * one(*cut)
    return factor_of


def scatter_about(own_key, extent, scale, most, cuts=(), kind=jnp.bfloat16):
    entries = jax.random.normal(own_key, extent, jnp.float32) * scale
    if len(cuts) > 0:
        entries = level_of(own_key, extent, cuts, -0.22, 0.18) * entries
    return jnp.clip(entries, min=-most, max=most).astype(kind)


def setup_inputs(seed: int = 0) -> dict:
    keys = jax.random.split(jax.random.key(seed), 8)
    positions = draw_positions(jax.random.fold_in(keys[7], 71), 0)
    velocities = draw_velocities(jax.random.fold_in(keys[7], 71), 0)
    accels = scatter_about(keys[2], (3, NSTARS), 0.05, 0.75, ((1, 32),), jnp.float32)
    jerks = scatter_about(keys[3], (3, NSTARS), 0.1, 1.5, ((1, 32),), jnp.float32)
    masses = jnp.clip(jnp.exp(math.log(3.0) - 2.3025851 * jax.random.uniform(keys[4], (NSTARS,), jnp.float32) ** level_of(keys[4], (NSTARS,), ((0, 32),), -0.2, 0.2)), 0.3, 3.0)
    elapsed = jnp.clip(jnp.exp(math.log(0.5) - 2.3025851 * jax.random.uniform(keys[5], (NSTARS,), jnp.float32) ** level_of(keys[5], (NSTARS,), ((0, 32),), -0.2, 0.2)), 0.05, 0.5)
    active_star = draw_active_star(jax.random.fold_in(keys[7], 71), 0)
    return dict(positions=positions, velocities=velocities, accels=accels, jerks=jerks, masses=masses, elapsed=elapsed, active_star=active_star)


softening = 0.001

def predict(positions, velocities, accels, jerks, elapsed):
    timestep = elapsed[None, :]
    moved_pos = positions + timestep * (velocities + timestep * (0.5 * accels + timestep * jerks / 6.0))
    moved_vel = velocities + timestep * (accels + 0.5 * timestep * jerks)
    return (moved_pos, moved_vel)

def correct(old_pos, old_vel, old_acc, old_jerk, new_acc, new_jerk, timestep):
    halfstep = 0.5 * timestep
    twelfth = timestep * timestep / 12.0
    new_vel = old_vel + halfstep * (old_acc + new_acc) + twelfth * (old_jerk - new_jerk)
    new_pos = old_pos + halfstep * (old_vel + new_vel) + twelfth * (old_acc - new_acc)
    return (new_pos, new_vel)

def pair_sums(targets, sources, ceiling):
    jcount = sources.shape[1]
    blk_width = math.gcd(jcount, ceiling)
    jpieces = jnp.transpose(sources.reshape(7, jcount // blk_width, blk_width), (1, 0, 2))

    def advance(running, jpiece):
        separation = jpiece[0:3, None, :] - targets[0:3, :, None]
        rel_velocity = jpiece[3:6, None, :] - targets[3:6, :, None]
        radius_sq = lax.optimization_barrier(jnp.sum(separation * separation, axis=0)) + softening
        inverse = lax.rsqrt(radius_sq)
        weight = jpiece[6][None, :] * inverse * inverse * inverse
        closing = 3.0 * lax.optimization_barrier(jnp.sum(separation * rel_velocity, axis=0)) / radius_sq
        accel_sum = lax.optimization_barrier(jnp.sum(weight[None] * separation, axis=2))
        change = lax.optimization_barrier(jnp.sum(weight[None] * (rel_velocity - closing[None] * separation), axis=2))
        return (running + jnp.concatenate([accel_sum, change], axis=0), None)
    initial = jnp.zeros((6, targets.shape[1]), jnp.float32)
    summed, unused = lax.scan(advance, initial, jpieces)
    return summed

def reference(positions, velocities, accels, jerks, masses, elapsed, active_star):
    moved_pos, moved_vel = predict(positions, velocities, accels, jerks, elapsed)
    sources = jnp.concatenate([moved_pos, moved_vel, masses[None, :]], axis=0)
    targets = jnp.take(sources[0:6], active_star, axis=1)
    summed = pair_sums(targets, sources, 2048) * (1.0 / NSTARS)
    new_acc = summed[0:3]
    new_jerk = summed[3:6]
    timestep = jnp.take(elapsed, active_star)[None, :]
    new_pos, new_vel = correct(jnp.take(positions, active_star, axis=1), jnp.take(velocities, active_star, axis=1), jnp.take(accels, active_star, axis=1), jnp.take(jerks, active_star, axis=1), new_acc, new_jerk, timestep)
    return (positions.at[:, active_star].set(new_pos), velocities.at[:, active_star].set(new_vel), accels.at[:, active_star].set(new_acc), jerks.at[:, active_star].set(new_jerk))
```

```python
import functools

import jax
import jax.numpy as jnp
from jax import lax
from jax.experimental import pallas as pl
from jax.experimental.pallas import tpu as pltpu
from jax.sharding import PartitionSpec as P

softening = 0.001
LANES = 128
SUB = 8
AXES = ("row", "col")
VMEM = pl.BlockSpec(memory_space=pltpu.VMEM)
SMEM = pl.BlockSpec(memory_space=pltpu.SMEM)


def predict_body(pos, vel, acc, jerk, mass, elapsed, out):
    step = elapsed[...]
    moved_pos = pos[...] + step * (vel[...] + step * (0.5 * acc[...] + step * jerk[...] * (1.0 / 6.0)))
    moved_vel = vel[...] + step * (acc[...] + 0.5 * step * jerk[...])
    for tile in range(pos.shape[1] // LANES):
        lanes = slice(tile * LANES, (tile + 1) * LANES)
        out[7 * tile : 7 * tile + 3, :] = moved_pos[:, lanes]
        out[7 * tile + 3 : 7 * tile + 6, :] = moved_vel[:, lanes]
        out[7 * tile + 6 : 7 * tile + 7, :] = mass[:, lanes]


def splat_row(ref, row):
    return jnp.broadcast_to(ref[row : row + 1, :], (SUB, LANES))


def add_pairs(target, sums, source):
    sums = list(sums)
    for base in range(0, source.shape[0], 7):
        sep = [splat_row(source, base + k) - target[k] for k in range(3)]
        rel = [splat_row(source, base + 3 + k) - target[3 + k] for k in range(3)]
        radius_sq = (sep[0] * sep[0] + sep[1] * sep[1]) + (sep[2] * sep[2] + softening)
        inverse = lax.rsqrt(radius_sq)
        inverse_sq = inverse * inverse
        weight = (splat_row(source, base + 6) * inverse) * inverse_sq
        dot = (sep[0] * rel[0] + sep[1] * rel[1]) + sep[2] * rel[2]
        closing = (3.0 * inverse_sq) * dot
        for k in range(3):
            sums[k] = sums[k] + weight * sep[k]
            sums[3 + k] = sums[3 + k] + weight * (rel[k] - closing * sep[k])
    return sums


def zeros6():
    return [jnp.zeros((SUB, LANES), jnp.float32) for _ in range(6)]


def setup_body(base, active, own, count, rank, targets, sums):
    tiles = own.shape[0] // 7
    rows = max(SUB, tiles)
    sub_rows = lax.broadcasted_iota(jnp.int32, (rows, LANES), 0)
    sub_lanes = lax.broadcasted_iota(jnp.int32, (LANES, LANES), 0)
    lane_cols = lax.broadcasted_iota(jnp.int32, (LANES, LANES), 1)
    flags = jnp.zeros((rows, LANES), jnp.float32)
    for r in range(active.shape[0]):
        local = active[r : r + 1, :] - base[0]
        high = local >> 7
        high = jnp.where(high < tiles, high, -1)
        low = local & 127
        one = (sub_rows == high).astype(jnp.float32)
        two = (sub_lanes == low).astype(jnp.float32)
        flags = flags + lax.dot_general(
            one, two, (((1,), (1,)), ((), ())), preferred_element_type=jnp.float32
        )
    before = (sub_lanes < lane_cols).astype(jnp.float32)
    order = jnp.dot(flags, before, preferred_element_type=jnp.float32)
    in_row = jnp.sum(flags, axis=1, keepdims=True)
    for r in range(tiles - 1):
        order = order + jnp.where(sub_rows > r, in_row[r : r + 1, :], 0.0)
    rank[...] = jnp.where(flags > 0.5, order, -1.0)
    total = jnp.sum(flags).astype(jnp.int32)
    count[0] = (total + (SUB - 1)) // SUB
    slot = lax.broadcasted_iota(jnp.int32, (SUB, LANES), 0)

    def fill(c, carry):
        ids = (slot + c * SUB).astype(jnp.float32)
        hits = [ids == splat_row(rank, t) for t in range(tiles)]
        target = []
        for k in range(6):
            found = jnp.zeros((SUB, LANES), jnp.float32)
            for t in range(tiles):
                found = found + jnp.where(hits[t], splat_row(own, 7 * t + k), 0.0)
            value = jnp.broadcast_to(jnp.sum(found, axis=1, keepdims=True), (SUB, LANES))
            targets[c, k] = value
            target.append(value)
        for k, value in enumerate(add_pairs(target, zeros6(), own)):
            sums[c, k] = value
        return carry

    lax.fori_loop(0, count[0], fill, 0)


def force_body(count, targets, running, *rest):
    sources, sums = rest[:-1], rest[-1]

    def chunk(c, carry):
        target = [targets[c, k] for k in range(6)]
        now = [running[c, k] for k in range(6)]
        for source in sources:
            now = add_pairs(target, now, source)
        for k in range(6):
            sums[c, k] = now[k]
        return carry

    lax.fori_loop(0, count[0], chunk, 0)


def final_body(scale, pieces, count, targets, running, rank, *rest):
    sources = rest[:pieces]
    pos, vel, acc, jerk, elapsed = rest[pieces : pieces + 5]
    new_pos, new_vel, new_acc, new_jerk = rest[pieces + 5 : pieces + 9]
    landed = rest[pieces + 9]
    tiles = pos.shape[1] // LANES
    slot = lax.broadcasted_iota(jnp.int32, (SUB, LANES), 0)
    landed[...] = jnp.zeros(landed.shape, jnp.float32)

    def chunk(c, carry):
        target = [targets[c, k] for k in range(6)]
        now = [running[c, k] for k in range(6)]
        for source in sources:
            now = add_pairs(target, now, source)
        ids = (slot + c * SUB).astype(jnp.float32)
        hits = [ids == splat_row(rank, t) for t in range(tiles)]
        for k in range(6):
            force = jnp.broadcast_to(jnp.sum(now[k], axis=1, keepdims=True), (SUB, LANES)) * scale
            for t in range(tiles):
                landed[t, k] += jnp.where(hits[t], force, 0.0)
        return carry

    lax.fori_loop(0, count[0], chunk, 0)
    for t in range(tiles):
        lanes = slice(t * LANES, (t + 1) * LANES)
        force = [jnp.sum(landed[t, k], axis=0, keepdims=True) for k in range(6)]
        acc_now = jnp.concatenate(force[0:3], axis=0)
        jerk_now = jnp.concatenate(force[3:6], axis=0)
        hit = jnp.broadcast_to(rank[t : t + 1, :], (3, LANES)) >= 0.0
        step = jnp.broadcast_to(elapsed[:, lanes], (3, LANES))
        half = 0.5 * step
        twelfth = step * step * (1.0 / 12.0)
        old_pos, old_vel = pos[:, lanes], vel[:, lanes]
        old_acc, old_jerk = acc[:, lanes], jerk[:, lanes]
        vel_now = old_vel + half * (old_acc + acc_now) + twelfth * (old_jerk - jerk_now)
        pos_now = old_pos + half * (old_vel + vel_now) + twelfth * (old_acc - acc_now)
        new_pos[:, lanes] = jnp.where(hit, pos_now, old_pos)
        new_vel[:, lanes] = jnp.where(hit, vel_now, old_vel)
        new_acc[:, lanes] = jnp.where(hit, acc_now, old_acc)
        new_jerk[:, lanes] = jnp.where(hit, jerk_now, old_jerk)


def partner(size, offset):
    if size & (size - 1) == 0:
        return [i ^ offset for i in range(size)]
    return [(i + offset) % size for i in range(size)]


def on_device(positions, velocities, accels, jerks, masses, elapsed, active_star):
    f32 = jnp.float32
    stars = positions.shape[1]
    row_count = lax.axis_size("row")
    col_count = lax.axis_size("col")
    device_id = lax.axis_index("row") * col_count + lax.axis_index("col")
    scale = 1.0 / (stars * row_count * col_count)
    cores = 2 if row_count % 2 == 0 else 1
    plane = row_count // cores

    def send(value, move):
        pairs = []
        for r in range(row_count):
            for c in range(col_count):
                p, q, z = move(r // cores, r % cores, c)
                pairs.append((r * col_count + c, (p * cores + q) * col_count + z))
        return lax.ppermute(value, AXES, pairs)

    def along_col(value, k):
        to = partner(col_count, k)
        return send(value, lambda p, q, z: (p, q, to[z]))

    def along_plane(value, k):
        to = partner(plane, k)
        return send(value, lambda p, q, z: (to[p], q, z))

    def across(value):
        return send(value, lambda p, q, z: (p, 1 - q, z))

    wide = elapsed.reshape(1, stars)
    tiles = stars // LANES
    slots = -(-stars // SUB)
    own = pl.pallas_call(
        predict_body,
        out_shape=jax.ShapeDtypeStruct((7 * tiles, LANES), f32),
        name="predict",
    )(positions, velocities, accels, jerks, masses.reshape(1, stars), wide)
    line = [own] + [along_col(own, k) for k in range(1, col_count)]

    block = jax.ShapeDtypeStruct((slots, 6, SUB, LANES), f32)
    count, rank, targets, sums = pl.pallas_call(
        setup_body,
        in_specs=[SMEM, VMEM, VMEM],
        out_shape=(
            jax.ShapeDtypeStruct((1,), jnp.int32),
            jax.ShapeDtypeStruct((max(SUB, tiles), LANES), f32),
            block,
            block,
        ),
        out_specs=(SMEM, VMEM, VMEM, VMEM),
        name="setup",
    )((device_id * stars).reshape(1).astype(jnp.int32), active_star.reshape(-1, LANES), own)

    def add_force(sums, *sources):
        return pl.pallas_call(
            force_body,
            in_specs=[SMEM] + [VMEM] * (2 + len(sources)),
            out_shape=block,
            out_specs=VMEM,
            input_output_aliases={2: 0},
            name="force",
        )(count, targets, sums, *sources)

    lined = jnp.concatenate(line, axis=0)
    planes = [along_plane(lined, k) for k in range(1, plane)]
    sums = add_force(sums, *line[1:])
    pieces = [lined] + planes
    for piece in planes:
        sums = add_force(sums, piece)
    if cores == 2:
        others = [across(piece) for piece in pieces]
        for piece in others[:-1]:
            sums = add_force(sums, piece)
        last = others[-1:]
    else:
        last = []

    shape = jax.ShapeDtypeStruct(positions.shape, f32)
    return pl.pallas_call(
        functools.partial(final_body, scale, len(last)),
        in_specs=[SMEM] + [VMEM] * (3 + len(last) + 5),
        out_shape=(shape, shape, shape, shape),
        out_specs=(VMEM, VMEM, VMEM, VMEM),
        scratch_shapes=[pltpu.VMEM((tiles, 6, SUB, LANES), f32)],
        name="final",
    )(count, targets, sums, rank, *last, positions, velocities, accels, jerks, wide)


def solution(mesh):
    whole = P(None, AXES)
    return jax.shard_map(
        on_device,
        mesh=mesh,
        in_specs=(whole, whole, whole, whole, P(AXES), P(AXES), P()),
        out_specs=(whole, whole, whole, whole),
        check_vma=False,
    )
```

```python
import functools

import jax
import jax.numpy as jnp
from jax import lax
from jax.experimental import pallas as pl
from jax.experimental.pallas import tpu as pltpu
from jax.sharding import PartitionSpec as P


softening = 0.001
LANES = 128
SUB = 8
AXES = ("row", "col")
VMEM = pl.BlockSpec(memory_space=pltpu.VMEM)
SMEM = pl.BlockSpec(memory_space=pltpu.SMEM)


PARAMS = pltpu.CompilerParams(vmem_limit_bytes=4 << 20)


def near(value):
    return pltpu.with_memory_space_constraint(value, pltpu.VMEM)


def far(value):
    return pltpu.with_memory_space_constraint(value, pltpu.HBM)


def predict_body(pos, vel, acc, jerk, mass, elapsed, out):
    step = elapsed[...]
    moved_pos = pos[...] + step * (vel[...] + step * (0.5 * acc[...] + step * jerk[...] * (1.0 / 6.0)))
    moved_vel = vel[...] + step * (acc[...] + 0.5 * step * jerk[...])
    for tile in range(pos.shape[1] // LANES):
        lanes = slice(tile * LANES, (tile + 1) * LANES)
        out[7 * tile : 7 * tile + 3, :] = moved_pos[:, lanes]
        out[7 * tile + 3 : 7 * tile + 6, :] = moved_vel[:, lanes]
        out[7 * tile + 6 : 7 * tile + 7, :] = mass[:, lanes]


def splat_row(ref, row):
    return jnp.broadcast_to(ref[row : row + 1, :], (SUB, LANES))


def add_pairs(target, sums, source):
    sums = list(sums)
    for base in range(0, source.shape[0], 7):
        sep = [splat_row(source, base + k) - target[k] for k in range(3)]
        rel = [splat_row(source, base + 3 + k) - target[3 + k] for k in range(3)]
        radius_sq = (sep[0] * sep[0] + sep[1] * sep[1]) + (sep[2] * sep[2] + softening)
        inverse = lax.rsqrt(radius_sq)
        inverse_sq = inverse * inverse
        weight = (splat_row(source, base + 6) * inverse) * inverse_sq
        dot = (sep[0] * rel[0] + sep[1] * rel[1]) + sep[2] * rel[2]
        closing = (3.0 * inverse_sq) * dot
        for k in range(3):
            sums[k] = sums[k] + weight * sep[k]
            sums[3 + k] = sums[3 + k] + weight * (rel[k] - closing * sep[k])
    return sums


def zeros6():
    return [jnp.zeros((SUB, LANES), jnp.float32) for _ in range(6)]


def setup_body(base, active, own, count, rank, targets, sums):
    tiles = own.shape[0] // 7
    rows = max(SUB, tiles)
    sub_rows = lax.broadcasted_iota(jnp.int32, (rows, LANES), 0)
    sub_lanes = lax.broadcasted_iota(jnp.int32, (LANES, LANES), 0)
    lane_cols = lax.broadcasted_iota(jnp.int32, (LANES, LANES), 1)
    flags = jnp.zeros((rows, LANES), jnp.float32)
    for r in range(active.shape[0]):
        local = active[r : r + 1, :] - base[0]
        high = local >> 7
        high = jnp.where(high < tiles, high, -1)
        low = local & 127
        one = (sub_rows == high).astype(jnp.float32)
        two = (sub_lanes == low).astype(jnp.float32)
        flags = flags + lax.dot_general(
            one, two, (((1,), (1,)), ((), ())), preferred_element_type=jnp.float32
        )
    before = (sub_lanes < lane_cols).astype(jnp.float32)
    order = jnp.dot(flags, before, preferred_element_type=jnp.float32)
    in_row = jnp.sum(flags, axis=1, keepdims=True)
    for r in range(tiles - 1):
        order = order + jnp.where(sub_rows > r, in_row[r : r + 1, :], 0.0)
    rank[...] = jnp.where(flags > 0.5, order, -1.0)
    total = jnp.sum(flags).astype(jnp.int32)
    count[0] = (total + (SUB - 1)) // SUB
    slot = lax.broadcasted_iota(jnp.int32, (SUB, LANES), 0)

    def fill(c, carry):
        ids = (slot + c * SUB).astype(jnp.float32)
        hits = [ids == splat_row(rank, t) for t in range(tiles)]
        target = []
        for k in range(6):
            found = jnp.zeros((SUB, LANES), jnp.float32)
            for t in range(tiles):
                found = found + jnp.where(hits[t], splat_row(own, 7 * t + k), 0.0)
            value = jnp.broadcast_to(jnp.sum(found, axis=1, keepdims=True), (SUB, LANES))
            targets[c, k] = value
            target.append(value)
        for k, value in enumerate(add_pairs(target, zeros6(), own)):
            sums[c, k] = value
        return carry

    lax.fori_loop(0, count[0], fill, 0)


def force_body(count, targets, running, *rest):
    sources, sums = rest[:-1], rest[-1]

    def chunk(c, carry):
        target = [targets[c, k] for k in range(6)]
        now = [running[c, k] for k in range(6)]
        for source in sources:
            now = add_pairs(target, now, source)
        for k in range(6):
            sums[c, k] = now[k]
        return carry

    lax.fori_loop(0, count[0], chunk, 0)


def final_body(scale, pieces, count, targets, running, rank, *rest):
    sources = rest[:pieces]
    pos, vel, acc, jerk, elapsed = rest[pieces : pieces + 5]
    new_pos, new_vel, new_acc, new_jerk = rest[pieces + 5 : pieces + 9]
    landed = rest[pieces + 9]
    tiles = pos.shape[1] // LANES
    slot = lax.broadcasted_iota(jnp.int32, (SUB, LANES), 0)
    landed[...] = jnp.zeros(landed.shape, jnp.float32)

    def chunk(c, carry):
        target = [targets[c, k] for k in range(6)]
        now = [running[c, k] for k in range(6)]
        for source in sources:
            now = add_pairs(target, now, source)
        ids = (slot + c * SUB).astype(jnp.float32)
        hits = [ids == splat_row(rank, t) for t in range(tiles)]
        for k in range(6):
            force = jnp.broadcast_to(jnp.sum(now[k], axis=1, keepdims=True), (SUB, LANES)) * scale
            for t in range(tiles):
                landed[t, k] += jnp.where(hits[t], force, 0.0)
        return carry

    lax.fori_loop(0, count[0], chunk, 0)
    for t in range(tiles):
        lanes = slice(t * LANES, (t + 1) * LANES)
        force = [jnp.sum(landed[t, k], axis=0, keepdims=True) for k in range(6)]
        acc_now = jnp.concatenate(force[0:3], axis=0)
        jerk_now = jnp.concatenate(force[3:6], axis=0)
        hit = jnp.broadcast_to(rank[t : t + 1, :], (3, LANES)) >= 0.0
        step = jnp.broadcast_to(elapsed[:, lanes], (3, LANES))
        half = 0.5 * step
        twelfth = step * step * (1.0 / 12.0)
        old_pos, old_vel = pos[:, lanes], vel[:, lanes]
        old_acc, old_jerk = acc[:, lanes], jerk[:, lanes]
        vel_now = old_vel + half * (old_acc + acc_now) + twelfth * (old_jerk - jerk_now)
        pos_now = old_pos + half * (old_vel + vel_now) + twelfth * (old_acc - acc_now)
        new_pos[:, lanes] = jnp.where(hit, pos_now, old_pos)
        new_vel[:, lanes] = jnp.where(hit, vel_now, old_vel)
        new_acc[:, lanes] = jnp.where(hit, acc_now, old_acc)
        new_jerk[:, lanes] = jnp.where(hit, jerk_now, old_jerk)


def partner(size, offset):
    if size & (size - 1) == 0:
        return [i ^ offset for i in range(size)]
    return [(i + offset) % size for i in range(size)]


def far_first(size):
    return list(range(size - 1, 0, -1))


def plan(plane, cores):
    pieces = [0] + far_first(plane)
    if cores == 1:
        return [("plane", k) for k in pieces[1:]]
    steps = [("core", 0)] + [("plane", k) for k in pieces[1:]]
    steps += [("core", k) for k in pieces[1:]]
    return steps


def on_device(positions, velocities, accels, jerks, masses, elapsed, active_star):
    f32 = jnp.float32
    stars = positions.shape[1]
    row_count = lax.axis_size("row")
    col_count = lax.axis_size("col")
    device_id = lax.axis_index("row") * col_count + lax.axis_index("col")
    scale = 1.0 / (stars * row_count * col_count)
    cores = 2 if row_count % 2 == 0 else 1
    plane = row_count // cores

    def send(value, move):
        pairs = []
        for r in range(row_count):
            for c in range(col_count):
                p, q, z = move(r // cores, r % cores, c)
                pairs.append((r * col_count + c, (p * cores + q) * col_count + z))
        return lax.ppermute(value, AXES, pairs)

    def along_col(value, k):
        to = partner(col_count, k)
        return send(value, lambda p, q, z: (p, q, to[z]))

    def along_plane(value, k):
        to = partner(plane, k)
        return send(value, lambda p, q, z: (to[p], q, z))

    def across(value):
        return send(value, lambda p, q, z: (p, 1 - q, z))

    wide = elapsed.reshape(1, stars)
    tiles = stars // LANES
    slots = -(-stars // SUB)
    own = pl.pallas_call(
        predict_body,
        out_shape=pltpu.VMEM((7 * tiles, LANES), f32),
        compiler_params=PARAMS,
        name="predict",
    )(*map(far, (positions, velocities, accels, jerks, masses.reshape(1, stars), wide)))
    line = [own] + [along_col(own, k) for k in far_first(col_count)]

    block = pltpu.VMEM((slots, 6, SUB, LANES), f32)
    count, rank, targets, sums = pl.pallas_call(
        setup_body,
        in_specs=[SMEM, VMEM, VMEM],
        out_shape=(
            pltpu.SMEM((1,), jnp.int32),
            pltpu.VMEM((max(SUB, tiles), LANES), f32),
            block,
            block,
        ),
        out_specs=(SMEM, VMEM, VMEM, VMEM),
        compiler_params=PARAMS,
        name="setup",
    )((device_id * stars).reshape(1).astype(jnp.int32), active_star.reshape(-1, LANES), near(own))

    def add_force(sums, *sources):
        return pl.pallas_call(
            force_body,
            in_specs=[SMEM] + [VMEM] * (2 + len(sources)),
            out_shape=block,
            out_specs=VMEM,
            input_output_aliases={2: 0},
            compiler_params=PARAMS,
            name="force",
        )(count, near(targets), near(sums), *map(near, sources))

    lined = jnp.concatenate(line, axis=0)
    pieces = {("plane", 0): lined}
    for k in far_first(plane):
        pieces["plane", k] = along_plane(lined, k)
    if cores == 2:
        for k in [0] + far_first(plane):
            pieces["core", k] = across(pieces["plane", k])
    sums = add_force(sums, *line[1:])
    steps = plan(plane, cores)
    for kind, k in steps[:-1]:
        sums = add_force(sums, pieces[kind, k])
    last = [pieces[step] for step in steps[-1:]]

    shape = jax.ShapeDtypeStruct(positions.shape, f32)
    return pl.pallas_call(
        functools.partial(final_body, scale, len(last)),
        in_specs=[SMEM] + [VMEM] * (3 + len(last) + 5),
        out_shape=(shape, shape, shape, shape),
        out_specs=(VMEM, VMEM, VMEM, VMEM),
        scratch_shapes=[pltpu.VMEM((tiles, 6, SUB, LANES), f32)],
        compiler_params=PARAMS,
        name="final",
    )(count, near(targets), near(sums), near(rank), *map(near, last), positions, velocities, accels, jerks, wide)


def solution(mesh):
    whole = P(None, AXES)

    return jax.shard_map(
        on_device,
        mesh=mesh,
        in_specs=(whole, whole, whole, whole, P(AXES), P(AXES), P()),
        out_specs=(whole, whole, whole, whole),
        check_vma=False,
    )
```

```python
import functools

import jax
import jax.numpy as jnp
from jax import lax
from jax.experimental import pallas as pl
from jax.experimental.pallas import tpu as pltpu
from jax.sharding import PartitionSpec as P


softening = 0.001
LANES = 128
SUB = 8
GROUP = 4
AXES = ("row", "col")
VMEM = pl.BlockSpec(memory_space=pltpu.VMEM)
SMEM = pl.BlockSpec(memory_space=pltpu.SMEM)


PARAMS = pltpu.CompilerParams(vmem_limit_bytes=4 << 20)


def near(value):
    return pltpu.with_memory_space_constraint(value, pltpu.VMEM)


def far(value):
    return pltpu.with_memory_space_constraint(value, pltpu.HBM)


def predict_body(pos, vel, acc, jerk, mass, elapsed, active, out, *kept):
    for source, copy in zip((pos, vel, acc, jerk, elapsed, active), kept):
        copy[...] = source[...]
    step = elapsed[...]
    moved_pos = pos[...] + step * (vel[...] + step * (0.5 * acc[...] + step * jerk[...] * (1.0 / 6.0)))
    moved_vel = vel[...] + step * (acc[...] + 0.5 * step * jerk[...])
    for tile in range(pos.shape[1] // LANES):
        lanes = slice(tile * LANES, (tile + 1) * LANES)
        out[7 * tile : 7 * tile + 3, :] = moved_pos[:, lanes]
        out[7 * tile + 3 : 7 * tile + 6, :] = moved_vel[:, lanes]
        out[7 * tile + 6 : 7 * tile + 7, :] = mass[:, lanes]


def splat_row(ref, row):
    return jnp.broadcast_to(ref[row : row + 1, :], (SUB, LANES))


def add_pairs(target, sums, source, first=0):
    sums = list(sums)
    for base in range(first, source.shape[0], 7):
        sep = [splat_row(source, base + k) - target[k] for k in range(3)]
        rel = [splat_row(source, base + 3 + k) - target[3 + k] for k in range(3)]
        radius_sq = (sep[0] * sep[0] + sep[1] * sep[1]) + (sep[2] * sep[2] + softening)
        inverse = lax.rsqrt(radius_sq)
        inverse_sq = inverse * inverse
        weight = (splat_row(source, base + 6) * inverse) * inverse_sq
        dot = (sep[0] * rel[0] + sep[1] * rel[1]) + sep[2] * rel[2]
        closing = (3.0 * inverse_sq) * dot
        for k in range(3):
            sums[k] = sums[k] + weight * sep[k]
            sums[3 + k] = sums[3 + k] + weight * (rel[k] - closing * sep[k])
    return sums


def zeros6():
    return [jnp.zeros((SUB, LANES), jnp.float32) for _ in range(6)]


def setup_body(base, active, own, near_by, count, rank, targets, sums):
    tiles = own.shape[0] // 7
    rows = max(SUB, tiles)
    sub_rows = lax.broadcasted_iota(jnp.int32, (rows, LANES), 0)
    sub_lanes = lax.broadcasted_iota(jnp.int32, (LANES, LANES), 0)
    lane_cols = lax.broadcasted_iota(jnp.int32, (LANES, LANES), 1)
    flags = jnp.zeros((rows, LANES), jnp.float32)
    for r in range(active.shape[0]):
        local = active[r : r + 1, :] - base[0]
        high = local >> 7
        high = jnp.where(high < tiles, high, -1)
        low = local & 127
        one = (sub_rows == high).astype(jnp.float32)
        two = (sub_lanes == low).astype(jnp.float32)
        flags = flags + lax.dot_general(
            one, two, (((1,), (1,)), ((), ())), preferred_element_type=jnp.float32
        )
    before = (sub_lanes < lane_cols).astype(jnp.float32)
    order = jnp.dot(flags, before, preferred_element_type=jnp.float32)
    in_row = jnp.sum(flags, axis=1, keepdims=True)
    for r in range(tiles - 1):
        order = order + jnp.where(sub_rows > r, in_row[r : r + 1, :], 0.0)
    rank[...] = jnp.where(flags > 0.5, order, -1.0)
    total = jnp.sum(flags).astype(jnp.int32)
    count[0] = (total + (SUB - 1)) // SUB
    slot = lax.broadcasted_iota(jnp.int32, (SUB, LANES), 0)
    lane = lax.broadcasted_iota(jnp.int32, (SUB, LANES), 1)

    def fill(c, carry):
        ids = (slot + c * SUB).astype(jnp.float32)
        hits = [ids == splat_row(rank, t) for t in range(tiles)]
        target = []
        packed = jnp.zeros((SUB, LANES), jnp.float32)
        for k in range(6):
            found = jnp.zeros((SUB, LANES), jnp.float32)
            for t in range(tiles):
                found = found + jnp.where(hits[t], splat_row(own, 7 * t + k), 0.0)
            value = jnp.broadcast_to(jnp.sum(found, axis=1, keepdims=True), (SUB, LANES))
            packed = jnp.where(lane == k, value, packed)
            target.append(value)
        targets[c] = packed
        for k, value in enumerate(add_pairs(target, zeros6(), near_by)):
            sums[c, k] = value
        return carry

    lax.fori_loop(0, count[0], fill, 0)


def add_piece(first, lead, count, targets, running, sent, got, sums):
    def unpack(c):
        packed = targets[c]
        return tuple(jnp.broadcast_to(packed[:, k : k + 1], (SUB, LANES)) for k in range(6))

    def add_from(source):
        def chunk(c, target):
            following = unpack(c + 1)
            now = add_pairs(target, [running[c, k] for k in range(6)], source, first)
            for k in range(6):
                sums[c, k] = now[k]
            return following

        lax.fori_loop(0, count[0], chunk, unpack(0))

    if got is None:
        add_from(sent)
        return

    @pl.when(lead[0] == 1)
    def from_link():
        add_from(sent)

    @pl.when(lead[0] != 1)
    def from_core():
        add_from(got)


def force_body(first, shared, lead, count, targets, running, *rest):
    sent, got, sums = (rest[0], rest[1], rest[2]) if shared else (rest[0], None, rest[1])
    add_piece(first, lead, count, targets, running, sent, got, sums)


def final_body(first, shared, scale, lead, count, targets, running, *rest):
    sent, got, rest = (rest[0], rest[1], rest[2:]) if shared else (rest[0], None, rest[1:])
    rank, pos, vel, acc, jerk, elapsed, new_pos, new_vel, new_acc, new_jerk, sums, landed = rest
    tiles = pos.shape[1] // LANES
    add_piece(first, lead, count, targets, running, sent, got, sums)
    slot = lax.broadcasted_iota(jnp.int32, (SUB, LANES), 0)
    landed[...] = jnp.zeros(landed.shape, jnp.float32)

    def land(g, carry):
        for c in range(GROUP):
            chunk = g * GROUP + c
            ids = (slot + chunk * SUB).astype(jnp.float32)
            hits = [ids == splat_row(rank, t) for t in range(tiles)]
            for k in range(6):
                total = jnp.sum(sums[chunk, k], axis=1, keepdims=True)
                force = jnp.broadcast_to(total, (SUB, LANES)) * scale
                for t in range(tiles):
                    landed[t, k] += jnp.where(hits[t], force, 0.0)
        return carry

    lax.fori_loop(0, (count[0] + (GROUP - 1)) // GROUP, land, 0)
    for t in range(tiles):
        lanes = slice(t * LANES, (t + 1) * LANES)
        force = [jnp.sum(landed[t, k], axis=0, keepdims=True) for k in range(6)]
        acc_now = jnp.concatenate(force[0:3], axis=0)
        jerk_now = jnp.concatenate(force[3:6], axis=0)
        hit = jnp.broadcast_to(rank[t : t + 1, :], (3, LANES)) >= 0.0
        step = jnp.broadcast_to(elapsed[:, lanes], (3, LANES))
        half = 0.5 * step
        twelfth = step * step * (1.0 / 12.0)
        old_pos, old_vel = pos[:, lanes], vel[:, lanes]
        old_acc, old_jerk = acc[:, lanes], jerk[:, lanes]
        vel_now = old_vel + half * (old_acc + acc_now) + twelfth * (old_jerk - jerk_now)
        pos_now = old_pos + half * (old_vel + vel_now) + twelfth * (old_acc - acc_now)
        new_pos[:, lanes] = jnp.where(hit, pos_now, old_pos)
        new_vel[:, lanes] = jnp.where(hit, vel_now, old_vel)
        new_acc[:, lanes] = jnp.where(hit, acc_now, old_acc)
        new_jerk[:, lanes] = jnp.where(hit, jerk_now, old_jerk)


def partner(size, offset):
    if size & (size - 1) == 0:
        return [i ^ offset for i in range(size)]
    return [(i + offset) % size for i in range(size)]


def sizes(mesh_shape):
    row_count, col_count = mesh_shape
    cores = 2 if row_count % 2 == 0 else 1
    return cores, row_count // cores, col_count


def col_order(count):
    middle = count // 2
    return ([middle] if middle > 1 else []) + [k for k in range(count - 1, 0, -1) if k != middle or k == 1]


def on_device(positions, velocities, accels, jerks, masses, elapsed, active_star):
    f32, i32 = jnp.float32, jnp.int32
    stars = positions.shape[1]
    row_count = lax.axis_size("row")
    col_count = lax.axis_size("col")
    row_index = lax.axis_index("row")
    device_id = row_index * col_count + lax.axis_index("col")
    scale = 1.0 / (stars * row_count * col_count)
    cores, plane, _ = sizes((row_count, col_count))

    def send(value, move):
        pairs = []
        for r in range(row_count):
            for c in range(col_count):
                p, q, z = move(r // cores, r % cores, c)
                pairs.append((r * col_count + c, (p * cores + q) * col_count + z))
        return lax.ppermute(value, AXES, pairs)

    def along_col(value, k):
        to = partner(col_count, k)
        idle = partner(plane, 1) if plane > 1 else None

        def move(p, q, z):
            if q == cores - 1 or idle is None:
                return p, q, to[z]
            return idle[p], q, z

        return send(value, move)

    def along_plane(value, k):
        to = partner(plane, k)
        idle = partner(col_count, 1) if col_count > 1 else None

        def move(p, q, z):
            if q == cores - 1 or idle is None:
                return to[p], q, z
            return p, q, idle[z]

        return send(value, move)

    def across(value):
        return send(value, lambda p, q, z: (p, 1 - q, z))

    wide = elapsed.reshape(1, stars)
    active = active_star.reshape(-1, LANES)
    tiles = stars // LANES
    slots = -(-stars // SUB)
    state = (positions, velocities, accels, jerks)
    own, *kept, wide, active = pl.pallas_call(
        predict_body,
        out_shape=(
            pltpu.VMEM((7 * tiles, LANES), f32),
            *(pltpu.VMEM(x.shape, f32) for x in state),
            pltpu.VMEM(wide.shape, f32),
            pltpu.VMEM(active.shape, i32),
        ),
        compiler_params=PARAMS,
        name="predict",
    )(*map(far, (*state, masses.reshape(1, stars), wide, active)))

    chip = jnp.concatenate([own, across(own)], axis=0) if cores == 2 else own
    found = [along_col(chip, k) for k in col_order(col_count)]

    block = pltpu.VMEM((slots, 6, SUB, LANES), f32)
    count, rank, targets, sums = pl.pallas_call(
        setup_body,
        in_specs=[SMEM, VMEM, VMEM, VMEM],
        out_shape=(
            pltpu.SMEM((1,), i32),
            pltpu.VMEM((max(SUB, tiles), LANES), f32),
            pltpu.VMEM((slots + 1, SUB, LANES), f32),
            block,
        ),
        out_specs=(SMEM, VMEM, VMEM, VMEM),
        compiler_params=PARAMS,
        name="setup",
    )((device_id * stars).reshape(1).astype(i32), near(active), near(own), near(chip))

    line = jnp.concatenate([chip, *found], axis=0)
    pieces = [("line", line, chip.shape[0])]
    pieces += [(f"plane_{k}", along_plane(line, k), 0) for k in range(1, plane)]
    shared = cores == 2
    lead = (row_index % cores == cores - 1).reshape(1).astype(i32)
    held = []
    for name, value, first in pieces:
        both = [value, across(value)] if shared else [value]
        held.append((name, first, both))
    for name, first, both in held[:-1]:
        sums = pl.pallas_call(
            functools.partial(force_body, first, shared),
            in_specs=[SMEM, SMEM] + [VMEM] * (2 + len(both)),
            out_shape=block,
            out_specs=VMEM,
            input_output_aliases={3: 0},
            compiler_params=PARAMS,
            name="force",
        )(lead, count, near(targets), near(sums), *map(near, both))

    name, first, both = held[-1]
    shape = jax.ShapeDtypeStruct(positions.shape, f32)
    near_args = (targets, sums, *both, rank, *kept, wide)
    return pl.pallas_call(
        functools.partial(final_body, first, shared, scale),
        in_specs=[SMEM, SMEM] + [VMEM] * len(near_args),
        out_shape=(shape, shape, shape, shape),
        out_specs=(VMEM, VMEM, VMEM, VMEM),
        scratch_shapes=[
            pltpu.VMEM((slots + GROUP, 6, SUB, LANES), f32),
            pltpu.VMEM((tiles, 6, SUB, LANES), f32),
        ],
        compiler_params=PARAMS,
        name="final",
    )(lead, count, *map(near, near_args))


def solution(mesh):
    whole = P(None, AXES)

    return jax.shard_map(
        on_device,
        mesh=mesh,
        in_specs=(whole, whole, whole, whole, P(AXES), P(AXES), P()),
        out_specs=(whole, whole, whole, whole),
        check_vma=False,
    )
```

```python
import functools

import jax
import jax.numpy as jnp
from jax import lax
from jax.experimental import pallas as pl
from jax.experimental.pallas import tpu as pltpu
from jax.sharding import PartitionSpec as P


softening = 0.001
LANES = 128
SUB = 8
GROUP = 4
AXES = ("row", "col")
VMEM = pl.BlockSpec(memory_space=pltpu.VMEM)
SMEM = pl.BlockSpec(memory_space=pltpu.SMEM)


PARAMS = pltpu.CompilerParams(vmem_limit_bytes=4 << 20)


def near(value):
    return pltpu.with_memory_space_constraint(value, pltpu.VMEM)


def far(value):
    return pltpu.with_memory_space_constraint(value, pltpu.HBM)


def predict_body(pos, vel, acc, jerk, mass, elapsed, active, out, *kept):
    for source, copy in zip((pos, vel, acc, jerk, elapsed, active), kept):
        copy[...] = source[...]
    step = elapsed[...]
    moved_pos = pos[...] + step * (vel[...] + step * (0.5 * acc[...] + step * jerk[...] * (1.0 / 6.0)))
    moved_vel = vel[...] + step * (acc[...] + 0.5 * step * jerk[...])
    for tile in range(pos.shape[1] // LANES):
        lanes = slice(tile * LANES, (tile + 1) * LANES)
        out[7 * tile : 7 * tile + 3, :] = moved_pos[:, lanes]
        out[7 * tile + 3 : 7 * tile + 6, :] = moved_vel[:, lanes]
        out[7 * tile + 6 : 7 * tile + 7, :] = mass[:, lanes]


def splat_row(ref, row):
    return jnp.broadcast_to(ref[row : row + 1, :], (SUB, LANES))


def add_pairs(target, sums, source):
    sums = list(sums)
    for base in range(0, source.shape[0], 7):
        sep = [splat_row(source, base + k) - target[k] for k in range(3)]
        rel = [splat_row(source, base + 3 + k) - target[3 + k] for k in range(3)]
        radius_sq = (sep[0] * sep[0] + sep[1] * sep[1]) + (sep[2] * sep[2] + softening)
        inverse = lax.rsqrt(radius_sq)
        inverse_sq = inverse * inverse
        weight = (splat_row(source, base + 6) * inverse) * inverse_sq
        dot = (sep[0] * rel[0] + sep[1] * rel[1]) + sep[2] * rel[2]
        closing = (3.0 * inverse_sq) * dot
        for k in range(3):
            sums[k] = sums[k] + weight * sep[k]
            sums[3 + k] = sums[3 + k] + weight * (rel[k] - closing * sep[k])
    return sums


def zeros6():
    return [jnp.zeros((SUB, LANES), jnp.float32) for _ in range(6)]


def setup_body(base, active, own, count, rank, targets):
    tiles = own.shape[0] // 7
    rows = max(SUB, tiles)
    sub_rows = lax.broadcasted_iota(jnp.int32, (rows, LANES), 0)
    sub_lanes = lax.broadcasted_iota(jnp.int32, (LANES, LANES), 0)
    lane_cols = lax.broadcasted_iota(jnp.int32, (LANES, LANES), 1)
    flags = jnp.zeros((rows, LANES), jnp.float32)
    for r in range(active.shape[0]):
        local = active[r : r + 1, :] - base[0]
        high = local >> 7
        high = jnp.where(high < tiles, high, -1)
        low = local & 127
        one = (sub_rows == high).astype(jnp.float32)
        two = (sub_lanes == low).astype(jnp.float32)
        flags = flags + lax.dot_general(
            one, two, (((1,), (1,)), ((), ())), preferred_element_type=jnp.float32
        )
    before = (sub_lanes < lane_cols).astype(jnp.float32)
    order = jnp.dot(flags, before, preferred_element_type=jnp.float32)
    in_row = jnp.sum(flags, axis=1, keepdims=True)
    for r in range(tiles - 1):
        order = order + jnp.where(sub_rows > r, in_row[r : r + 1, :], 0.0)
    rank[...] = jnp.where(flags > 0.5, order, -1.0)
    total = jnp.sum(flags).astype(jnp.int32)
    count[0] = (total + (SUB - 1)) // SUB
    slot = lax.broadcasted_iota(jnp.int32, (SUB, LANES), 0)

    def fill(c, carry):
        ids = (slot + c * SUB).astype(jnp.float32)
        hits = [ids == splat_row(rank, t) for t in range(tiles)]
        for k in range(6):
            found = jnp.zeros((SUB, LANES), jnp.float32)
            for t in range(tiles):
                found = found + jnp.where(hits[t], splat_row(own, 7 * t + k), 0.0)
            targets[c, k] = jnp.broadcast_to(jnp.sum(found, axis=1, keepdims=True), (SUB, LANES))
        return carry

    lax.fori_loop(0, count[0], fill, 0)


def add_pieces(count, targets, running, sources, sums):
    def chunk(c, carry):
        target = [targets[c, k] for k in range(6)]
        now = zeros6() if running is None else [running[c, k] for k in range(6)]
        for source in sources:
            now = add_pairs(target, now, source)
        for k in range(6):
            sums[c, k] = now[k]
        return carry

    lax.fori_loop(0, count[0], chunk, 0)


def first_body(count, targets, *rest):
    add_pieces(count, targets, None, rest[:-1], rest[-1])


def force_body(count, targets, running, *rest):
    add_pieces(count, targets, running, rest[:-1], rest[-1])


def final_body(scale, count, targets, running, source, rank, pos, vel, acc, jerk, elapsed, *rest):
    new_pos, new_vel, new_acc, new_jerk, sums, landed = rest
    tiles = pos.shape[1] // LANES
    add_pieces(count, targets, running, [source], sums)
    slot = lax.broadcasted_iota(jnp.int32, (SUB, LANES), 0)
    landed[...] = jnp.zeros(landed.shape, jnp.float32)

    def land(g, carry):
        for c in range(GROUP):
            chunk = g * GROUP + c
            ids = (slot + chunk * SUB).astype(jnp.float32)
            hits = [ids == splat_row(rank, t) for t in range(tiles)]
            for k in range(6):
                total = jnp.sum(sums[chunk, k], axis=1, keepdims=True)
                force = jnp.broadcast_to(total, (SUB, LANES)) * scale
                for t in range(tiles):
                    landed[t, k] += jnp.where(hits[t], force, 0.0)
        return carry

    lax.fori_loop(0, (count[0] + (GROUP - 1)) // GROUP, land, 0)
    for t in range(tiles):
        lanes = slice(t * LANES, (t + 1) * LANES)
        force = [jnp.sum(landed[t, k], axis=0, keepdims=True) for k in range(6)]
        acc_now = jnp.concatenate(force[0:3], axis=0)
        jerk_now = jnp.concatenate(force[3:6], axis=0)
        hit = jnp.broadcast_to(rank[t : t + 1, :], (3, LANES)) >= 0.0
        step = jnp.broadcast_to(elapsed[:, lanes], (3, LANES))
        half = 0.5 * step
        twelfth = step * step * (1.0 / 12.0)
        old_pos, old_vel = pos[:, lanes], vel[:, lanes]
        old_acc, old_jerk = acc[:, lanes], jerk[:, lanes]
        vel_now = old_vel + half * (old_acc + acc_now) + twelfth * (old_jerk - jerk_now)
        pos_now = old_pos + half * (old_vel + vel_now) + twelfth * (old_acc - acc_now)
        new_pos[:, lanes] = jnp.where(hit, pos_now, old_pos)
        new_vel[:, lanes] = jnp.where(hit, vel_now, old_vel)
        new_acc[:, lanes] = jnp.where(hit, acc_now, old_acc)
        new_jerk[:, lanes] = jnp.where(hit, jerk_now, old_jerk)


def partner(size, offset):
    if size & (size - 1) == 0:
        return [i ^ offset for i in range(size)]
    return [(i + offset) % size for i in range(size)]


def sizes(mesh_shape):
    row_count, col_count = mesh_shape
    cores = 2 if row_count % 2 == 0 else 1
    return cores, row_count // cores, col_count


def col_slots(count, cores):
    if cores == 1:
        return [(k, None) for k in range(1, count)]
    near_by = list(range(1, (count - 1) // 2 + 1))
    distant = list(range(len(near_by) + 1, count))
    return list(zip(distant, near_by + [None] * (len(distant) - len(near_by))))


def on_device(positions, velocities, accels, jerks, masses, elapsed, active_star):
    f32, i32 = jnp.float32, jnp.int32
    stars = positions.shape[1]
    row_count = lax.axis_size("row")
    col_count = lax.axis_size("col")
    row_index = lax.axis_index("row")
    device_id = row_index * col_count + lax.axis_index("col")
    scale = 1.0 / (stars * row_count * col_count)
    cores, plane, _ = sizes((row_count, col_count))

    def send(value, move):
        pairs = []
        for r in range(row_count):
            for c in range(col_count):
                p, q, z = move(r // cores, r % cores, c)
                pairs.append((r * col_count + c, (p * cores + q) * col_count + z))
        return lax.ppermute(value, AXES, pairs)

    def along_col(value, ours, theirs):
        idle = partner(plane, 1) if plane > 1 else None

        def move(p, q, z):
            k = ours if q == cores - 1 else theirs
            if k is not None:
                return p, q, partner(col_count, k)[z]
            if idle is None:
                return p, q, partner(col_count, 1)[z]
            return idle[p], q, z

        return send(value, move)

    def along_plane(value, k):
        to = partner(plane, k)
        return send(value, lambda p, q, z: (to[p], q, z))

    def across(value):
        return send(value, lambda p, q, z: (p, 1 - q, z))

    wide = elapsed.reshape(1, stars)
    active = active_star.reshape(-1, LANES)
    tiles = stars // LANES
    slots = -(-stars // SUB)
    state = (positions, velocities, accels, jerks)
    own, *kept, wide, active = pl.pallas_call(
        predict_body,
        out_shape=(
            pltpu.VMEM((7 * tiles, LANES), f32),
            *(pltpu.VMEM(x.shape, f32) for x in state),
            pltpu.VMEM(wide.shape, f32),
            pltpu.VMEM(active.shape, i32),
        ),
        compiler_params=PARAMS,
        name="predict",
    )(*map(far, (*state, masses.reshape(1, stars), wide, active)))

    lead = row_index % cores == cores - 1
    chip = jnp.concatenate([own, across(own)], axis=0) if cores == 2 else own
    slots = col_slots(col_count, cores)
    half = [along_col(chip, ours, theirs) for ours, theirs in slots]
    if cores == 2 and slots and slots[-1][1] is None:
        half[-1] = jnp.where(lead, half[-1], chip)
    else:
        half = [own, *half]

    block = pltpu.VMEM((-(-stars // SUB), 6, SUB, LANES), f32)
    count, rank, targets = pl.pallas_call(
        setup_body,
        in_specs=[SMEM, VMEM, VMEM],
        out_shape=(
            pltpu.SMEM((1,), i32),
            pltpu.VMEM((max(SUB, tiles), LANES), f32),
            block,
        ),
        out_specs=(SMEM, VMEM, VMEM),
        compiler_params=PARAMS,
        name="setup",
    )((device_id * stars).reshape(1).astype(i32), near(active), near(own))

    half = jnp.concatenate(half, axis=0)
    held = {"half": half}
    held.update({f"plane_{k}": along_plane(half, k) for k in plane_order(plane)})
    if cores == 2:
        held.update({f"core_{name}": across(value) for name, value in list(held.items())})
    order = add_order(plane, cores)
    sums = None
    for name in order[:-1]:
        args = (targets, held[name]) if sums is None else (targets, sums, held[name])
        sums = pl.pallas_call(
            first_body if sums is None else force_body,
            in_specs=[SMEM] + [VMEM] * len(args),
            out_shape=block,
            out_specs=VMEM,
            input_output_aliases={} if sums is None else {2: 0},
            compiler_params=PARAMS,
            name="force",
        )(count, *map(near, args))

    shape = jax.ShapeDtypeStruct(positions.shape, f32)
    if sums is None:
        sums = jnp.zeros(block.shape, f32)
    near_args = (targets, sums, held[order[-1]], rank, *kept, wide)
    return pl.pallas_call(
        functools.partial(final_body, scale),
        in_specs=[SMEM] + [VMEM] * len(near_args),
        out_shape=(shape, shape, shape, shape),
        out_specs=(VMEM, VMEM, VMEM, VMEM),
        scratch_shapes=[
            pltpu.VMEM((block.shape[0] + GROUP, 6, SUB, LANES), f32),
            pltpu.VMEM((tiles, 6, SUB, LANES), f32),
        ],
        compiler_params=PARAMS,
        name="final",
    )(count, *map(near, near_args))


def plane_order(plane):
    return list(range(2, plane)) + ([1] if plane > 1 else [])


def add_order(plane, cores):
    planes = [f"plane_{k}" for k in plane_order(plane)]
    if cores == 1:
        return ["half", *planes]
    order = ["half", "core_half"]
    for i, name in enumerate(planes):
        order.append(name)
        if i + 1 < len(planes):
            order.append(f"core_{name}")
    if len(planes) > 1:
        order[-2:] = [f"core_{planes[-2]}", planes[-1]]
    return order + [f"core_{name}" for name in planes[-1:]]


def solution(mesh):
    whole = P(None, AXES)

    return jax.shard_map(
        on_device,
        mesh=mesh,
        in_specs=(whole, whole, whole, whole, P(AXES), P(AXES), P()),
        out_specs=(whole, whole, whole, whole),
        check_vma=False,
    )
```

```python
import functools

import jax
import jax.numpy as jnp
from jax import lax
from jax.experimental import pallas as pl
from jax.experimental.pallas import tpu as pltpu
from jax.sharding import PartitionSpec as P


softening = 0.001
LANES = 128
SUB = 8
GROUP = 4
AXES = ("row", "col")
VMEM = pl.BlockSpec(memory_space=pltpu.VMEM)
SMEM = pl.BlockSpec(memory_space=pltpu.SMEM)


PARAMS = pltpu.CompilerParams(vmem_limit_bytes=4 << 20)


def near(value):
    return pltpu.with_memory_space_constraint(value, pltpu.VMEM)


def far(value):
    return pltpu.with_memory_space_constraint(value, pltpu.HBM)


def predict_body(pos, vel, acc, jerk, mass, elapsed, active, out, *kept):
    for source, copy in zip((pos, vel, acc, jerk, elapsed, active), kept):
        copy[...] = source[...]
    step = elapsed[...]
    moved_pos = pos[...] + step * (vel[...] + step * (0.5 * acc[...] + step * jerk[...] * (1.0 / 6.0)))
    moved_vel = vel[...] + step * (acc[...] + 0.5 * step * jerk[...])
    for tile in range(pos.shape[1] // LANES):
        lanes = slice(tile * LANES, (tile + 1) * LANES)
        out[7 * tile : 7 * tile + 3, :] = moved_pos[:, lanes]
        out[7 * tile + 3 : 7 * tile + 6, :] = moved_vel[:, lanes]
        out[7 * tile + 6 : 7 * tile + 7, :] = mass[:, lanes]


def splat_row(ref, row):
    return jnp.broadcast_to(ref[row : row + 1, :], (SUB, LANES))


def add_pairs(target, sums, source):
    sums = list(sums)
    for base in range(0, source.shape[0], 7):
        sep = [splat_row(source, base + k) - target[k] for k in range(3)]
        rel = [splat_row(source, base + 3 + k) - target[3 + k] for k in range(3)]
        radius_sq = (sep[0] * sep[0] + sep[1] * sep[1]) + (sep[2] * sep[2] + softening)
        inverse = lax.rsqrt(radius_sq)
        inverse_sq = inverse * inverse
        weight = (splat_row(source, base + 6) * inverse) * inverse_sq
        dot = (sep[0] * rel[0] + sep[1] * rel[1]) + sep[2] * rel[2]
        closing = (3.0 * inverse_sq) * dot
        for k in range(3):
            sums[k] = sums[k] + weight * sep[k]
            sums[3 + k] = sums[3 + k] + weight * (rel[k] - closing * sep[k])
    return sums


def zeros6():
    return [jnp.zeros((SUB, LANES), jnp.float32) for _ in range(6)]


def setup_body(base, active, own, count, rank, targets):
    tiles = own.shape[0] // 7
    rows = max(SUB, tiles)
    sub_rows = lax.broadcasted_iota(jnp.int32, (rows, LANES), 0)
    sub_lanes = lax.broadcasted_iota(jnp.int32, (LANES, LANES), 0)
    lane_cols = lax.broadcasted_iota(jnp.int32, (LANES, LANES), 1)
    flags = jnp.zeros((rows, LANES), jnp.float32)
    for r in range(active.shape[0]):
        local = active[r : r + 1, :] - base[0]
        high = local >> 7
        high = jnp.where(high < tiles, high, -1)
        low = local & 127
        one = (sub_rows == high).astype(jnp.float32)
        two = (sub_lanes == low).astype(jnp.float32)
        flags = flags + lax.dot_general(
            one, two, (((1,), (1,)), ((), ())), preferred_element_type=jnp.float32
        )
    before = (sub_lanes < lane_cols).astype(jnp.float32)
    order = jnp.dot(flags, before, preferred_element_type=jnp.float32)
    in_row = jnp.sum(flags, axis=1, keepdims=True)
    for r in range(tiles - 1):
        order = order + jnp.where(sub_rows > r, in_row[r : r + 1, :], 0.0)
    rank[...] = jnp.where(flags > 0.5, order, -1.0)
    total = jnp.sum(flags).astype(jnp.int32)
    count[0] = (total + (SUB - 1)) // SUB
    slot = lax.broadcasted_iota(jnp.int32, (SUB, LANES), 0)

    def fill(c, carry):
        ids = (slot + c * SUB).astype(jnp.float32)
        hits = [ids == splat_row(rank, t) for t in range(tiles)]
        for k in range(6):
            found = jnp.zeros((SUB, LANES), jnp.float32)
            for t in range(tiles):
                found = found + jnp.where(hits[t], splat_row(own, 7 * t + k), 0.0)
            targets[c, k] = jnp.broadcast_to(jnp.sum(found, axis=1, keepdims=True), (SUB, LANES))
        return carry

    lax.fori_loop(0, count[0], fill, 0)


def add_pieces(count, targets, running, sources, sums):
    def chunk(c, carry):
        target = [targets[c, k] for k in range(6)]
        now = zeros6() if running is None else [running[c, k] for k in range(6)]
        for source in sources:
            now = add_pairs(target, now, source)
        for k in range(6):
            sums[c, k] = now[k]
        return carry

    lax.fori_loop(0, count[0], chunk, 0)


def line_body(shared, lead, count, targets, running, swapped, fetched, sums):
    @pl.when(lead[0] == 1)
    def on_lead():
        add_pieces(count, targets, running, [swapped.at[0:shared], fetched], sums)

    @pl.when(lead[0] != 1)
    def on_other():
        add_pieces(count, targets, running, [swapped], sums)


def first_body(count, targets, *rest):
    add_pieces(count, targets, None, rest[:-1], rest[-1])


def force_body(count, targets, running, *rest):
    add_pieces(count, targets, running, rest[:-1], rest[-1])


def final_body(scale, count, targets, running, source, rank, pos, vel, acc, jerk, elapsed, *rest):
    new_pos, new_vel, new_acc, new_jerk, sums, landed = rest
    tiles = pos.shape[1] // LANES
    add_pieces(count, targets, running, [source], sums)
    slot = lax.broadcasted_iota(jnp.int32, (SUB, LANES), 0)
    landed[...] = jnp.zeros(landed.shape, jnp.float32)

    def land(g, carry):
        forces, hits = [], []
        for c in range(GROUP):
            chunk = g * GROUP + c
            ids = (slot + chunk * SUB).astype(jnp.float32)
            hits.append([ids == splat_row(rank, t) for t in range(tiles)])
            sides = [jnp.sum(sums[chunk, k], axis=1, keepdims=True) for k in range(6)]
            forces.append([jnp.broadcast_to(side, (SUB, LANES)) for side in sides])
        for k in range(6):
            for t in range(tiles):
                found = [jnp.where(hits[c][t], forces[c][k], 0.0) for c in range(GROUP)]
                landed[t, k] += functools.reduce(jnp.add, found)
        return carry

    lax.fori_loop(0, (count[0] + (GROUP - 1)) // GROUP, land, 0)
    for t in range(tiles):
        lanes = slice(t * LANES, (t + 1) * LANES)
        force = [jnp.sum(landed[t, k], axis=0, keepdims=True) * scale for k in range(6)]
        acc_now = jnp.concatenate(force[0:3], axis=0)
        jerk_now = jnp.concatenate(force[3:6], axis=0)
        hit = jnp.broadcast_to(rank[t : t + 1, :], (3, LANES)) >= 0.0
        step = jnp.broadcast_to(elapsed[:, lanes], (3, LANES))
        half = 0.5 * step
        twelfth = step * step * (1.0 / 12.0)
        old_pos, old_vel = pos[:, lanes], vel[:, lanes]
        old_acc, old_jerk = acc[:, lanes], jerk[:, lanes]
        vel_now = old_vel + half * (old_acc + acc_now) + twelfth * (old_jerk - jerk_now)
        pos_now = old_pos + half * (old_vel + vel_now) + twelfth * (old_acc - acc_now)
        new_pos[:, lanes] = jnp.where(hit, pos_now, old_pos)
        new_vel[:, lanes] = jnp.where(hit, vel_now, old_vel)
        new_acc[:, lanes] = jnp.where(hit, acc_now, old_acc)
        new_jerk[:, lanes] = jnp.where(hit, jerk_now, old_jerk)


def partner(size, offset):
    if size & (size - 1) == 0:
        return [i ^ offset for i in range(size)]
    return [(i + offset) % size for i in range(size)]


def sizes(mesh_shape):
    row_count, col_count = mesh_shape
    cores = 2 if row_count % 2 == 0 else 1
    return cores, row_count // cores, col_count


def col_slots(count, cores):
    if cores == 1:
        return [(k, None) for k in range(1, count)]
    near_by = list(range(1, (count - 1) // 2 + 1))
    distant = list(range(len(near_by) + 1, count))
    return list(zip(distant, near_by + [None] * (len(distant) - len(near_by))))


def on_device(positions, velocities, accels, jerks, masses, elapsed, active_star):
    f32, i32 = jnp.float32, jnp.int32
    stars = positions.shape[1]
    row_count = lax.axis_size("row")
    col_count = lax.axis_size("col")
    row_index = lax.axis_index("row")
    device_id = row_index * col_count + lax.axis_index("col")
    scale = 1.0 / (stars * row_count * col_count)
    cores, plane, _ = sizes((row_count, col_count))

    def send(value, move):
        pairs = []
        for r in range(row_count):
            for c in range(col_count):
                p, q, z = move(r // cores, r % cores, c)
                pairs.append((r * col_count + c, (p * cores + q) * col_count + z))
        return lax.ppermute(value, AXES, pairs)

    def along_col(value, ours, theirs):
        idle = partner(plane, 1) if plane > 1 else None
        crossed = cores == 2 and col_count >= 4 and col_count & (col_count - 1) == 0

        def move(p, q, z):
            k = ours if q == cores - 1 else theirs
            if crossed and q == cores - 1 and z >= col_count // 2:
                k = ours ^ 1
            if k is not None:
                return p, q, partner(col_count, k)[z]
            if idle is None:
                return p, q, partner(col_count, 1)[z]
            return idle[p], q, z

        return send(value, move)

    def along_plane(value, k):
        to = partner(plane, k)
        return send(value, lambda p, q, z: (to[p], q, z))

    def across(value):
        return send(value, lambda p, q, z: (p, 1 - q, z))

    wide = elapsed.reshape(1, stars)
    active = active_star.reshape(-1, LANES)
    tiles = stars // LANES
    slots = -(-stars // SUB)
    state = (positions, velocities, accels, jerks)
    own, *kept, wide, active = pl.pallas_call(
        predict_body,
        out_shape=(
            pltpu.VMEM((7 * tiles, LANES), f32),
            *(pltpu.VMEM(x.shape, f32) for x in state),
            pltpu.VMEM(wide.shape, f32),
            pltpu.VMEM(active.shape, i32),
        ),
        compiler_params=PARAMS,
        name="predict",
    )(*map(far, (*state, masses.reshape(1, stars), wide, active)))

    lead = row_index % cores == cores - 1
    chip = jnp.concatenate([own, across(own)], axis=0) if cores == 2 else own
    slots = col_slots(col_count, cores)
    fetched = [along_col(chip, ours, theirs) for ours, theirs in slots]
    split = cores == 2 and len(slots) > 0 and slots[-1][1] is None
    if split:
        first = [chip, *fetched[:-1]]
        half = [*fetched[:-1], jnp.where(lead, fetched[-1], chip)]
    else:
        first = half = [own, *fetched]

    block = pltpu.VMEM((-(-stars // SUB), 6, SUB, LANES), f32)
    count, rank, targets = pl.pallas_call(
        setup_body,
        in_specs=[SMEM, VMEM, VMEM],
        out_shape=(
            pltpu.SMEM((1,), i32),
            pltpu.VMEM((max(SUB, tiles), LANES), f32),
            block,
        ),
        out_specs=(SMEM, VMEM, VMEM),
        compiler_params=PARAMS,
        name="setup",
    )((device_id * stars).reshape(1).astype(i32), near(active), near(own))

    half = jnp.concatenate(half, axis=0)
    held = {"half": half}
    held.update({f"plane_{k}": along_plane(half, k) for k in plane_order(plane)})
    if cores == 2:
        held.update({f"core_{name}": across(value) for name, value in list(held.items())})

    def add(body, sums, *sources, flags=()):
        args = (targets, *sources) if sums is None else (targets, sums, *sources)
        return pl.pallas_call(
            body,
            in_specs=[SMEM] * (1 + len(flags)) + [VMEM] * len(args),
            out_shape=block,
            out_specs=VMEM,
            input_output_aliases={} if sums is None else {2 + len(flags): 0},
            compiler_params=PARAMS,
            name="force",
        )(*flags, count, *map(near, args))

    sums = add(first_body, None, *first)
    order = add_order(plane, cores)
    for name in order[:-1]:
        if name == "core_half" and split:
            flag = lead.reshape(1).astype(i32)
            shared = half.shape[0] - chip.shape[0]
            body = functools.partial(line_body, shared)
            sums = add(body, sums, held[name], fetched[-1], flags=(flag,))
        else:
            sums = add(force_body, sums, held[name])

    shape = jax.ShapeDtypeStruct(positions.shape, f32)
    near_args = (targets, sums, held[order[-1]], rank, *kept, wide)
    return pl.pallas_call(
        functools.partial(final_body, scale),
        in_specs=[SMEM] + [VMEM] * len(near_args),
        out_shape=(shape, shape, shape, shape),
        out_specs=(VMEM, VMEM, VMEM, VMEM),
        scratch_shapes=[
            pltpu.VMEM((block.shape[0] + GROUP, 6, SUB, LANES), f32),
            pltpu.VMEM((tiles, 6, SUB, LANES), f32),
        ],
        compiler_params=PARAMS,
        name="final",
    )(count, *map(near, near_args))


def plane_order(plane):
    return list(range(2, plane)) + ([1] if plane > 1 else [])


def add_order(plane, cores):
    planes = [f"plane_{k}" for k in plane_order(plane)]
    if cores == 1:
        return planes
    order = ["core_half"]
    for i, name in enumerate(planes):
        order.append(name)
        if i + 1 < len(planes):
            order.append(f"core_{name}")
    if len(planes) > 1:
        order[-2:] = [f"core_{planes[-2]}", planes[-1]]
    return order + [f"core_{name}" for name in planes[-1:]]


def solution(mesh):
    whole = P(None, AXES)

    return jax.shard_map(
        on_device,
        mesh=mesh,
        in_specs=(whole, whole, whole, whole, P(AXES), P(AXES), P()),
        out_specs=(whole, whole, whole, whole),
        check_vma=False,
    )
```
